32 devices in a mesh: groups: 2 (over y), ep: 16 (over z, x, core).
Axes of the slice: x: 2, y: 2, z: 4, core: 2. Of those that a mesh axis runs over, the one named last changes fastest.
Arguments:
- tokens: bfloat16 [128, 7168], P(('groups', 'ep')), parts along dimension 0, may hold values from -6 to 6
- routes: int32 [128, 8], P(('groups', 'ep')), parts along dimension 0, may hold values from 0 to 15, as said below
- gates: float32 [128, 8], P(('groups', 'ep')), parts along dimension 0, may hold values from 0.05 to 0.6
- gate_weight: bfloat16 [7168, 32768], P(None, 'ep'), may hold values from -0.0625 to 0.0625
- up_weight: bfloat16 [7168, 32768], P(None, 'ep'), may hold values from -0.0625 to 0.0625
- down_weight: bfloat16 [32768, 7168], P('ep'), may hold values from -0.125 to 0.125
Outputs:
- mixed: bfloat16 [128, 7168], P(('groups', 'ep')), parts along dimension 0
The draws below stay inside these ranges and needn't reach their ends.
There are 2 independent parts, one for each index of `groups`. The reference program is written for one: setup_inputs(seed, part) draws one part's arguments, and reference() takes and returns one part's arrays. A program takes and returns all parts, laid end to end along the dimension named above; an argument that names none is the same for every part. Nothing has to cross between parts.
Inputs may be any that keep to these rules, and one draw needn't show every extreme that they name: `routes`: each token names 8 different experts. Among the 4 tokens of one device no expert is named by more than 3 of them, and in every draw one expert is named by exactly 3 tokens of every device.
All inputs are finite; a program needn't handle non-finite values.
Results may differ from the reference program's by a relative error of at most 0.0085.
Values may be sent and summed in bfloat16 or wider, within the bound.
No kernel may reach another device: no remote copies, remote signals or barrier semaphores. Data moves between devices by JAX's collectives and lax.ppermute only.
A program may use at most 128 MiB of HBM per device.

```python
import math
import jax
import jax.numpy as jnp
from jax import lax

D = 7168
FF = 2048
TOP = 8
EXPERTS = 16
TOK_DEV = 4
CAP = 3
TOKENS = 64


def draw_routes(key, part):
    hot_expert = jax.random.randint(jax.random.fold_in(key, 11), (), 0, EXPERTS).astype(jnp.int32)
    blocks = TOKENS // TOK_DEV
    block_keys = jax.random.split(jax.random.fold_in(key, 12), blocks)
    others = (hot_expert + 1 + jnp.arange(EXPERTS - 1, dtype=jnp.int32)) % EXPERTS
    expert_pool = jnp.repeat(others, CAP)

    def one_block(block_key):
        key_pool, key_rows, key_cols = jax.random.split(block_key, 3)
        shuffled = expert_pool[jax.random.permutation(key_pool, expert_pool.shape[0])]
        chosen = jnp.concatenate([jnp.full((CAP,), hot_expert, jnp.int32), shuffled[:TOK_DEV * TOP - CAP]])
        ordered = jnp.sort(chosen)
        route_table = ordered.reshape(TOP, TOK_DEV).T
        route_table = route_table[jax.random.permutation(key_rows, TOK_DEV)]
        scores = jax.random.randint(key_cols, (TOK_DEV, TOP), 0, 1 << 20) * TOP + jnp.arange(TOP, dtype=jnp.int32)[None, :]
        return jnp.take_along_axis(route_table, jnp.argsort(scores, axis=1), axis=1)
    return jax.vmap(one_block)(block_keys).reshape(TOKENS, TOP).astype(jnp.int32)


def level_of(rng, dims, cuts, low, top_value):
    level = 1.0
    for dim, blocks in cuts:
        draws = jax.random.uniform(jax.random.fold_in(jax.random.fold_in(rng, 6), dim), (blocks,), jnp.float32, low / len(cuts), top_value / len(cuts))
        level = level * jnp.repeat(jnp.exp(draws), dims[dim] // blocks).reshape((-1,) + (1,) * (len(dims) - 1 - dim))
    return level


def gaussian(key, dims, deviation, most, cuts=(), kind=jnp.bfloat16):
    gain = level_of(key, dims, cuts, -0.22, 0.18) if cuts else 1.0
    entries = jax.random.normal(key, dims, jnp.float32) * deviation * gain
    return jnp.minimum(jnp.maximum(entries, -most), most).astype(kind)


def setup_inputs(seed: int = 0, part: int = 0) -> dict:
    streams_of = jax.random.split(jax.random.key(seed), 7)
    part_splits = jax.random.split(jax.random.fold_in(streams_of[6], part), 7)
    return {
        "tokens": gaussian(part_splits[0], (TOKENS, D), 1.0, 6.0, ((0, 16),)),
        "routes": draw_routes(jax.random.fold_in(jax.random.fold_in(streams_of[6], part), 71), part),
        "gates": jnp.clip(jnp.exp(math.log(0.6) - 2.4849067 * jax.random.uniform(part_splits[2], (TOKENS, TOP), jnp.float32) ** level_of(part_splits[2], (TOKENS, TOP), ((0, 16),), -0.2, 0.2)), 0.05, 0.6),
        "gate_weight": gaussian(streams_of[3], (D, EXPERTS * FF), D ** -0.5, 0.0625, ((1, 16),)),
        "up_weight": gaussian(streams_of[4], (D, EXPERTS * FF), D ** -0.5, 0.0625, ((1, 16),)),
        "down_weight": gaussian(streams_of[5], (EXPERTS * FF, D), FF ** -0.5, 0.125, ((0, 16),)),
    }


def reference(tokens, routes, gates, gate_weight, up_weight, down_weight):
    bound = CAP * (TOKENS // TOK_DEV)

    def add_expert(running, expert):
        matches = routes == expert
        routed = jnp.any(matches, axis=1)
        weight = jnp.sum(jnp.where(matches, gates, jnp.zeros_like(gates)), axis=1)
        row_order = jnp.argsort(jnp.where(routed, 0, 1).astype(jnp.int32), stable=True)[:bound].astype(jnp.int32)
        picked_rows = tokens[row_order]
        start = (expert * FF).astype(jnp.int32)
        gate_cols = lax.dynamic_slice_in_dim(gate_weight, start, FF, 1)
        up_cols = lax.dynamic_slice_in_dim(up_weight, start, FF, 1)
        down_rows = lax.dynamic_slice_in_dim(down_weight, start, FF, 0)
        gate_act = jnp.dot(picked_rows, gate_cols, preferred_element_type=jnp.float32)
        up_act = jnp.dot(picked_rows, up_cols, preferred_element_type=jnp.float32)
        hidden = (jax.nn.silu(gate_act) * up_act).astype(jnp.bfloat16)
        expert_out = jnp.dot(hidden, down_rows, preferred_element_type=jnp.float32)
        running = running.at[row_order].add(weight[row_order][:, None] * expert_out)
        return running, None

    initial = jnp.zeros(tokens.shape, jnp.float32)
    running, unused = lax.scan(add_expert, initial, jnp.arange(EXPERTS, dtype=jnp.int32))
    return running.astype(jnp.bfloat16)
```

```python
import jax
import jax.numpy as jnp
from jax import lax
from jax.experimental import pallas as pl
from jax.experimental.pallas import tpu as pltpu
from jax.sharding import PartitionSpec as P


EXPERTS = 16
LANES = 128
UNIT = 512


def load_kernel(source, target, sems):
    count, _, unit = target.shape
    copies = [
        pltpu.make_async_copy(source.at[:, pl.ds(j * unit, unit)], target.at[j], sems.at[j])
        for j in range(count)
    ]
    for copy in copies:
        copy.start()
    for copy in copies:
        copy.wait()


def load_columns(weight, count):
    return pl.pallas_call(
        load_kernel,
        out_shape=pltpu.VMEM((count, weight.shape[0], UNIT), weight.dtype),
        in_specs=[pl.BlockSpec(memory_space=pltpu.HBM)],
        out_specs=pl.BlockSpec(memory_space=pltpu.VMEM),
        scratch_shapes=[pltpu.SemaphoreType.DMA((count,))],
        compiler_params=pltpu.CompilerParams(vmem_limit_bytes=1 << 20),
    )(weight)


def join_kernel(*refs):
    target = refs[-1]
    size = target.shape[0] // (len(refs) - 1)
    for i, part in enumerate(refs[:-1]):
        target[pl.ds(i * size, size)] = part[...]


def join(parts):
    vmem = pl.BlockSpec(memory_space=pltpu.VMEM)
    return pl.pallas_call(
        join_kernel,
        out_shape=pltpu.VMEM((sum(p.shape[0] for p in parts), parts[0].shape[1]), parts[0].dtype),
        in_specs=[vmem] * len(parts),
        out_specs=vmem,
        compiler_params=pltpu.CompilerParams(vmem_limit_bytes=2 << 20),
    )(*[pltpu.with_memory_space_constraint(part, pltpu.VMEM) for part in parts])


def gate_of(info, expert):
    lane = lax.broadcasted_iota(jnp.int32, info.shape, 1)
    return jnp.sum(jnp.where(lane % EXPERTS == expert, info.astype(jnp.float32), 0.0), axis=1, keepdims=True)


def expert_kernel(
    per_expert, pieces, gate_in, up_in, gate_hbm, down_hbm, send, keep, gate_held, up_held, rows, hidden, last_sem, sems
):
    del gate_in, up_in
    units, kept = up_held.shape[0], gate_held.shape[0]
    depth, width = down_hbm.shape
    half = send.shape[0]
    chunks = width // UNIT
    per_unit = gate_held.shape[1] // depth
    model = rows.shape[1]
    last = pltpu.make_async_copy(gate_hbm.at[:, pl.ds(kept * UNIT, UNIT)], gate_held.at[0], last_sem)
    freed = [(up_held, 0)] + [(held, j) for j in range(1, kept) for held in (gate_held, up_held)]

    def place(c):
        held, j = freed[c // per_unit]
        return held.at[j, pl.ds((c % per_unit) * depth, depth)]

    downs = [
        pltpu.make_async_copy(down_hbm.at[:, pl.ds(c * UNIT, UNIT)], place(c), sems.at[c])
        for c in range(chunks)
    ]
    info = []
    for i, piece in enumerate(pieces):
        rows[pl.ds(i * piece.shape[0], piece.shape[0])] = piece[:, :model]
        info.append(piece[:, model:])
    expert = lax.axis_index("ep") // per_expert
    gate = jnp.concatenate([gate_of(part, expert) for part in info], axis=0)
    started = 0
    for j in range(units):
        if j == kept:
            last.wait()
        x = rows[...]
        gate_act = jnp.dot(x, gate_held[j % kept], preferred_element_type=jnp.float32)
        up_act = jnp.dot(x, up_held[j], preferred_element_type=jnp.float32)
        value = gate_act / (1.0 + jnp.exp(-gate_act)) * up_act
        hidden[:, pl.ds(j * UNIT, UNIT)] = value.astype(hidden.dtype)
        if j == 0:
            last.start()
        for c in range(started, min((2 * j + 1) * per_unit, chunks)):
            downs[c].start()
            started = c + 1
    for c in range(chunks):
        downs[c].wait()
        part = jnp.dot(hidden[...], place(c)[...], preferred_element_type=jnp.float32) * gate
        keep[:, pl.ds(c * UNIT, UNIT)] = part[:half].astype(keep.dtype)
        send[:, pl.ds(c * UNIT, UNIT)] = part[half:].astype(send.dtype)


def run_expert(per_expert, pieces, gate_held, up_held, gate_weight, down_weight):
    count = len(pieces)
    total = sum(piece.shape[0] for piece in pieces)
    half, width = total // 2, down_weight.shape[1]

    def kernel(*refs):
        expert_kernel(per_expert, refs[:count], *refs[count:])

    vmem = pl.BlockSpec(memory_space=pltpu.VMEM)
    hbm = pl.BlockSpec(memory_space=pltpu.HBM)
    held = [pltpu.with_memory_space_constraint(piece, pltpu.VMEM) for piece in pieces]
    outs = pl.pallas_call(
        kernel,
        out_shape=(
            pltpu.VMEM((half, width), jnp.bfloat16),
            pltpu.VMEM((half, width), jnp.float32),
            pltpu.VMEM(gate_held.shape, gate_held.dtype),
            pltpu.VMEM(up_held.shape, up_held.dtype),
        ),
        in_specs=[vmem] * (count + 2) + [hbm, hbm],
        out_specs=(vmem,) * 4,
        input_output_aliases={count: 2, count + 1: 3},
        scratch_shapes=[
            pltpu.VMEM((total, gate_held.shape[1]), jnp.bfloat16),
            pltpu.VMEM((total, down_weight.shape[0]), jnp.bfloat16),
            pltpu.SemaphoreType.DMA,
            pltpu.SemaphoreType.DMA((width // UNIT,)),
        ],
        compiler_params=pltpu.CompilerParams(vmem_limit_bytes=3 << 20),
    )(*held, gate_held, up_held, gate_weight, down_weight)
    return outs[0], outs[1]


def plain_expert(per_expert, rows, gate_weight, up_weight, down_weight):
    model = gate_weight.shape[0]
    x = rows[:, :model]
    gate_act = jnp.dot(x, gate_weight, preferred_element_type=jnp.float32)
    up_act = jnp.dot(x, up_weight, preferred_element_type=jnp.float32)
    hidden = (jax.nn.silu(gate_act) * up_act).astype(jnp.bfloat16)
    part = jnp.dot(hidden, down_weight, preferred_element_type=jnp.float32)
    part = part * gate_of(rows[:, model:], lax.axis_index("ep") // per_expert)
    half = part.shape[0] // 2
    return part[half:].astype(jnp.bfloat16), part[:half]


def with_gates(tokens, routes, gates):
    member = routes[:, :, None] == jnp.arange(EXPERTS, dtype=jnp.int32)
    share = jnp.sum(jnp.where(member, gates[:, :, None], 0.0), axis=1)
    high = lax.reduce_precision(share, 8, 7)
    middle = lax.reduce_precision(share - high, 8, 7)
    low = share - high - middle
    parts = jnp.concatenate([high, middle, low], axis=1).astype(jnp.bfloat16)
    info = jnp.pad(parts, ((0, 0), (0, LANES - parts.shape[1])))
    return jnp.concatenate([tokens, info], axis=1)


def stages_of(devices):
    bits = []
    bit = devices // 2
    while bit >= 1:
        bits.append(bit)
        bit //= 2
    stages = []
    while len(bits) > 2:
        take = min(2, len(bits) - 2)
        group, bits = bits[:take], bits[take:]
        stages.append(tuple(sorted((sum(b for i, b in enumerate(group) if m >> i & 1) for m in range(1, 2 ** len(group))), reverse=True)))
    return stages + [(b,) for b in bits]


def shards(tokens, routes, gates, gate_weight, up_weight, down_weight):
    devices = lax.axis_size("ep")
    per_expert = devices // EXPERTS

    def swap(x, offset):
        return lax.ppermute(x, "ep", [(i, i ^ offset) for i in range(devices)])

    stages = stages_of(devices)
    depth, hidden = gate_weight.shape[0], gate_weight.shape[1]
    units = hidden // UNIT
    fast = hidden == 4 * UNIT and devices * tokens.shape[0] <= 64 and depth % UNIT == 0
    rows = with_gates(tokens, routes, gates)
    for offsets in stages[:-2]:
        parts = [rows] + [swap(rows, offset) for offset in offsets]
        rows = join(parts) if fast else jnp.concatenate(parts, axis=0)
    pieces = [rows, swap(rows, stages[-2][0])]
    pieces += [swap(piece, stages[-1][0]) for piece in pieces]
    if fast:
        gate_weight, up_weight, down_weight = (
            pltpu.with_memory_space_constraint(w, pltpu.HBM) for w in (gate_weight, up_weight, down_weight)
        )
        gate_held = load_columns(gate_weight, units - 1)
        up_held = load_columns(up_weight, units)
        send, keep = run_expert(per_expert, pieces, gate_held, up_held, gate_weight, down_weight)
    else:
        rows = jnp.concatenate(pieces, axis=0)
        send, keep = plain_expert(per_expert, rows, gate_weight, up_weight, down_weight)
    keep = keep + swap(send, stages[-1][0]).astype(jnp.float32)
    for offsets in stages[-2::-1]:
        size = keep.shape[0] // (len(offsets) + 1)
        got = [
            swap(keep[(i + 1) * size : (i + 2) * size].astype(jnp.bfloat16), offset)
            for i, offset in enumerate(offsets)
        ]
        keep = keep[:size] + sum(part.astype(jnp.float32) for part in got)
    return keep.astype(jnp.bfloat16)


def solution(mesh):
    placed = (
        P(("groups", "ep"), None),
        P(("groups", "ep"), None),
        P(("groups", "ep"), None),
        P(None, "ep"),
        P(None, "ep"),
        P("ep", None),
    )

    return jax.shard_map(shards, mesh=mesh, in_specs=placed, out_specs=P(("groups", "ep"), None), check_vma=False)
```
